32 devices in a mesh: lat: 8 (over y, x, core), lon: 4 (over z).
Axes of the slice: x: 2, y: 2, z: 4, core: 2. Of those that a mesh axis runs over, the one named last changes fastest.
Arguments:
- velocity: bfloat16 [16, 1024, 512], P(None, 'lat', 'lon'), may hold values from -6 to 6
- theta: bfloat16 [16, 1024, 512], P(None, 'lat', 'lon'), may hold values from -6 to 6
- dx_cell: float32 [1024, 512], P('lat', 'lon'), may hold values from 0.5 to 2
- wet_levels: int32 [1024, 512], P('lat', 'lon'), may hold values from 0 to 16
- bottom_index: int32 [1024, 512], P('lat', 'lon'), may hold values from 1 to 4
- basin_id: int32 [1024, 512], P('lat', 'lon'), may hold values from 0 to 9
- layer_dz: float32 [16], replicated, may hold values from 0.5 to 2
Outputs:
- overturning: float32 [2, 10, 16, 1024], P(None, None, 'lon', 'lat')
The draws below stay inside these ranges and needn't reach their ends.
All inputs are finite; a program needn't handle non-finite values.
Results may differ from the reference program's by a relative error of at most 0.0003.
Values sent between devices are 32-bit elements; how exact they have to be, the bound alone decides.
No kernel may reach another device: no remote copies, remote signals or barrier semaphores. Data moves between devices by JAX's collectives and lax.ppermute only.
A program may use at most 64 MiB of HBM per device.

```python
import math
import jax
import jax.numpy as jnp
from jax import lax

BASINS = 10
NY = 1024
NX = 512
LEV = 16


def set_ends(array, stream_key, low, largest):
    longest = array.shape.index(max(array.shape))
    spots = []
    for shift in (0, 1):
        where = [jax.random.randint(jax.random.fold_in(stream_key, axis), (), 0, length) for axis, length in enumerate(array.shape)]
        where[longest] = (where[longest] + shift) % array.shape[longest]
        spots.append(tuple(where))
    return array.at[spots[0]].set(low).at[spots[1]].set(largest)


def raised(entries, rng, source, target, blocks, factor):
    def block_of(position):
        return (jnp.arange(entries.shape[position]) // (entries.shape[position] // blocks)).reshape((-1,) + (1,) * (entries.ndim - 1 - position))

    near = jax.random.permutation(rng, blocks)[block_of(target)]
    other_side = (block_of(target) + blocks // 2) % blocks
    return jnp.where((block_of(source) == near) | (block_of(source) == other_side), factor * entries, entries)


def shard_levels(key, extent, pieces, smallest, top_value):
    loudness, own = 1.0, jax.random.fold_in(key, 6)
    for position, parts in pieces:
        draws = jnp.exp(jax.random.uniform(jax.random.fold_in(own, position), (parts,), jnp.float32, smallest / len(pieces), top_value / len(pieces)))
        loudness = loudness * jnp.repeat(draws, extent[position] // parts).reshape([-1 if axis == position else 1 for axis in range(len(extent))])
    return loudness


def bell_draw(stream_key, dims, scale, bound, shards=(), kind=jnp.bfloat16):
    values = jax.random.normal(stream_key, dims, jnp.float32) * scale
    if len(shards) > 0:
        values = shard_levels(stream_key, dims, shards, -0.22, 0.18) * values
    return jnp.clip(values, min=-bound, max=bound).astype(kind)


def gaussian_with(stream_key, shape, width, most, shards, heavy, kind=jnp.bfloat16):
    entries = width * jax.random.normal(stream_key, shape, jnp.float32)
    if shards:
        entries = entries * shard_levels(stream_key, shape, shards, -0.22, 0.18)
    return jnp.clip(raised(entries, jax.random.fold_in(stream_key, 3), *heavy), -most, most).astype(kind)


def setup_inputs(seed: int = 0) -> dict:
    seeds = jax.random.split(jax.random.key(seed), 8)
    velocity = gaussian_with(seeds[0], (LEV, NY, NX), 1.0, 6.0, ((1, 8), (2, 4)), (2, 0, 4, 2.0))
    theta = bell_draw(seeds[1], (LEV, NY, NX), 1.0, 6.0, ((1, 8), (2, 4)))
    dx_cell = jnp.clip(jnp.exp(math.log(2.0) - 1.3862944 * jax.random.uniform(seeds[2], (NY, NX), jnp.float32) ** shard_levels(seeds[2], (NY, NX), ((0, 8), (1, 4)), -0.2, 0.2)), 0.5, 2.0)
    wet_levels = set_ends(jax.random.randint(seeds[3], (NY, NX), 0, LEV + 1), jax.random.fold_in(seeds[3], 1), 0, LEV).astype(jnp.int32)
    bottom_index = set_ends(jax.random.randint(seeds[4], (NY, NX), 1, 5), jax.random.fold_in(seeds[4], 1), 1, 4).astype(jnp.int32)
    basin_id = set_ends(jax.random.randint(seeds[5], (NY, NX), 0, BASINS), jax.random.fold_in(seeds[5], 1), 0, BASINS - 1).astype(jnp.int32)
    layer_dz = jnp.clip(jnp.exp(jax.random.uniform(seeds[6], (LEV,), jnp.float32, math.log(0.5), math.log(2.0))), 0.5, 2.0)
    return {"velocity": velocity, "theta": theta, "dx_cell": dx_cell, "wet_levels": wet_levels, "bottom_index": bottom_index, "basin_id": basin_id, "layer_dz": layer_dz}


def reference(velocity, theta, dx_cell, wet_levels, bottom_index, basin_id, layer_dz):
    bottom_part = bottom_index.astype(jnp.float32) * 0.25

    def one_level(items):
        level, velocity_level, theta_level, thick_top = items
        wet_cells = (level < wet_levels).astype(jnp.float32)
        bottom_cells = level == wet_levels - 1
        thick = thick_top * jnp.where(bottom_cells, bottom_part, jnp.float32(1.0)) * wet_cells
        volume = velocity_level.astype(jnp.float32) * thick * dx_cell
        heat = volume * theta_level.astype(jnp.float32)
        vol_rows = jnp.stack([jnp.sum(jnp.where(basin_id == basin, volume, jnp.float32(0.0)), axis=1) for basin in range(BASINS)])
        heat_rows = jnp.stack([jnp.sum(jnp.where(basin_id == basin, heat, jnp.float32(0.0)), axis=1) for basin in range(BASINS)])
        return jnp.stack([vol_rows, heat_rows])

    levels = jnp.arange(LEV, dtype=jnp.int32)
    zonal = lax.map(one_level, (levels, velocity, theta, layer_dz))
    cumulated = jnp.cumsum(zonal, axis=0) * jnp.float32(1.0 / (NX ** 0.5))
    return jnp.transpose(cumulated, (1, 2, 0, 3))
```

```python
import functools

import jax
import jax.numpy as jnp
from jax import lax
from jax.experimental import pallas as pl
from jax.experimental.pallas import tpu as pltpu
from jax.sharding import PartitionSpec as P

BASINS = 10
SUBLANES = 8


def zonal_kernel(
    scale, owners, per_owner,
    dz_ref, velocity_hbm, theta_hbm, dx_hbm, wet_hbm, bottom_hbm, basin_hbm,
    out_ref,
    velocity_in, theta_in, dx_in, wet_in, bottom_in, basin_in,
    dx_t, dxb_t, wet_t, basin_t, running, sems,
):
    rows, columns = dx_in.shape
    column_vregs = columns // SUBLANES
    fields = 2
    lines = fields * BASINS * per_owner

    def static_copy(source, target, index):
        return pltpu.make_async_copy(source, target, sems.at[index])

    static_copies = [
        static_copy(dx_hbm, dx_in, 0),
        static_copy(bottom_hbm, bottom_in, 1),
        static_copy(wet_hbm, wet_in, 2),
        static_copy(basin_hbm, basin_in, 3),
    ]

    def level_copies(owner):
        span = pl.ds(owner * per_owner, per_owner)
        return [
            pltpu.make_async_copy(velocity_hbm.at[span], velocity_in.at[span], sems.at[4 + 2 * owner]),
            pltpu.make_async_copy(theta_hbm.at[span], theta_in.at[span], sems.at[5 + 2 * owner]),
        ]

    for copy in static_copies:
        copy.start()
    for owner in range(owners):
        for copy in level_copies(owner):
            copy.start()
    for copy in static_copies:
        copy.wait()
    dx = dx_in[...]
    dx_t[...] = jnp.transpose(dx)
    dxb_t[...] = jnp.transpose(dx * (bottom_in[...].astype(jnp.float32) * 0.25))
    wet_t[...] = jnp.transpose(wet_in[...])
    basin_t[...] = jnp.transpose(basin_in[...])

    def one_owner(owner, sums):
        for copy in level_copies(owner):
            copy.wait()
        sums = list(sums)
        for local in range(per_owner):
            level = owner * per_owner + local
            thick_top = dz_ref[level] * scale
            velocity_t = jnp.transpose(velocity_in[level].astype(jnp.float32))
            theta_t = jnp.transpose(theta_in[level].astype(jnp.float32))
            for column in range(column_vregs):
                part = slice(column * SUBLANES, (column + 1) * SUBLANES)
                wet = wet_t[part, :]
                width = jnp.where(
                    wet > level + 1,
                    dx_t[part, :],
                    jnp.where(wet == level + 1, dxb_t[part, :], jnp.float32(0.0)),
                )
                volume = velocity_t[part, :] * (width * thick_top)
                heat = volume * theta_t[part, :]
                basin = basin_t[part, :]
                for b in range(BASINS):
                    here = basin == b
                    sums[b] = sums[b] + jnp.where(here, volume, jnp.float32(0.0))
                    sums[BASINS + b] = sums[BASINS + b] + jnp.where(here, heat, jnp.float32(0.0))
            for fb in range(fields * BASINS):
                running[pl.ds((fb * per_owner + local) * SUBLANES, SUBLANES), :] = sums[fb]
        for first in range(0, lines, SUBLANES):
            total = running[pl.ds(first * SUBLANES, SUBLANES, stride=SUBLANES), :]
            for sublane in range(1, SUBLANES):
                total = total + running[pl.ds(first * SUBLANES + sublane, SUBLANES, stride=SUBLANES), :]
            out_ref[owner, pl.ds(first, SUBLANES), :] = total
        return tuple(sums)

    zero = jnp.zeros((SUBLANES, rows), jnp.float32)
    lax.fori_loop(0, owners, one_owner, (zero,) * (fields * BASINS))


def local_running(scale, owners, velocity, theta, dx_cell, wet_levels, bottom_index, basin_id, layer_dz):
    levels, rows, columns = velocity.shape
    per_owner = levels // owners
    lines = 2 * BASINS * per_owner
    hbm = pl.BlockSpec(memory_space=pl.ANY)
    flat = (rows, columns)
    turned = (columns, rows)
    return pl.pallas_call(
        functools.partial(zonal_kernel, scale, owners, per_owner),
        out_shape=jax.ShapeDtypeStruct((owners, lines, rows), jnp.float32),
        in_specs=[pl.BlockSpec(memory_space=pltpu.SMEM)] + [hbm] * 6,
        out_specs=pl.BlockSpec(memory_space=pltpu.VMEM),
        scratch_shapes=[
            pltpu.VMEM(velocity.shape, velocity.dtype),
            pltpu.VMEM(theta.shape, theta.dtype),
            pltpu.VMEM(flat, jnp.float32),
            pltpu.VMEM(flat, jnp.int32),
            pltpu.VMEM(flat, jnp.int32),
            pltpu.VMEM(flat, jnp.int32),
            pltpu.VMEM(turned, jnp.float32),
            pltpu.VMEM(turned, jnp.float32),
            pltpu.VMEM(turned, jnp.int32),
            pltpu.VMEM(turned, jnp.int32),
            pltpu.VMEM((lines * SUBLANES, rows), jnp.float32),
            pltpu.SemaphoreType.DMA((4 + 2 * owners,)),
        ],
        name="zonal",
    )(layer_dz, velocity, theta, dx_cell, wet_levels, bottom_index, basin_id)


def on_device(owners, velocity, theta, dx_cell, wet_levels, bottom_index, basin_id, layer_dz):
    levels, rows, columns = velocity.shape
    scale = 1.0 / (columns * owners) ** 0.5
    pieces = local_running(
        scale, owners, velocity, theta, dx_cell, wet_levels, bottom_index, basin_id, layer_dz
    )
    me = lax.axis_index("lon")
    total = lax.dynamic_index_in_dim(pieces, me, 0, False)
    for step in range(1, owners):
        piece = lax.dynamic_index_in_dim(pieces, (me + step) % owners, 0, False)
        total = total + lax.ppermute(piece, "lon", [(i, (i + step) % owners) for i in range(owners)])
    return total.reshape(2, BASINS, levels // owners, rows)


def solution(mesh):
    placed = (
        P(None, "lat", "lon"),
        P(None, "lat", "lon"),
        P("lat", "lon"),
        P("lat", "lon"),
        P("lat", "lon"),
        P("lat", "lon"),
        P(),
    )
    return jax.shard_map(
        functools.partial(on_device, mesh.shape["lon"]),
        mesh=mesh,
        in_specs=placed,
        out_specs=P(None, None, "lon", "lat"),
        check_vma=False,
    )
```

```python
import functools

import jax
import jax.numpy as jnp
from jax import lax
from jax.experimental import pallas as pl
from jax.experimental.pallas import tpu as pltpu
from jax.sharding import PartitionSpec as P


BASINS = 10
FIELDS = 2
SUBLANES = 8
LEVEL_GROUP = 2
KERNEL_VMEM = 16 * 1024 * 1024


def exchange_plan(owners):
    ring = list(range(0, owners, 2)) + list(range(1, owners, 2))
    shifts = []
    for distance in range(1, owners // 2 + 1):
        shifts += sorted({distance, owners - distance})
    sends = [
        [(ring[place], ring[(place + shift) % owners]) for place in range(owners)] for shift in shifts
    ]
    pieces = [[dict(pairs)[device] for device in range(owners)] for pairs in sends]
    return sends, pieces + [list(range(owners))]


def looked_up(table, me):
    found = jnp.int32(table[0])
    for device in range(1, len(table)):
        found = jnp.where(me == device, jnp.int32(table[device]), found)
    return found


def add_above(owner, per_owner, state, above, sums_ref, wait):
    velocity_in, theta_in, _, _, _, basin_t, dz_wide, dx_in, dxb_in, wet_in = state
    rows, columns = dx_in.shape
    block = 2 * SUBLANES
    for field in range(FIELDS):
        above[field] = jnp.zeros((rows, columns), jnp.float32)

    def add_owner(upper, carry):
        wait(upper)
        for row in range(0, rows, block):
            part = slice(row, row + block)
            wet, dx, dxb = wet_in[part, :], dx_in[part, :], dxb_in[part, :]
            volumes, heats = above[0, part, :], above[1, part, :]
            for local in range(per_owner):
                level = upper * per_owner + local
                width = jnp.where(
                    wet > level + 1, dx, jnp.where(wet == level + 1, dxb, jnp.float32(0.0))
                )
                volume = velocity_in[level, part, :].astype(jnp.float32) * (width * dz_wide[level, 0:1, 0:1])
                volumes += volume
                heats += volume * theta_in[level, part, :].astype(jnp.float32)
            above[0, part, :] = volumes
            above[1, part, :] = heats
        return carry

    lax.fori_loop(0, owner, add_owner, 0)
    sums = [jnp.zeros((SUBLANES, rows), jnp.float32)] * (FIELDS * BASINS)
    flows = [jnp.transpose(above[field]) for field in range(FIELDS)]
    for column in range(0, columns, SUBLANES):
        part = slice(column, column + SUBLANES)
        for b in range(BASINS):
            here = basin_t[part, :] == b
            for field in range(FIELDS):
                sums[field * BASINS + b] += jnp.where(here, flows[field][part, :], jnp.float32(0.0))
    save_sums(sums_ref, sums)


def one_piece(owner, per_owner, sums, state, running, piece_ref):
    velocity_in, theta_in, dx_t, dxb_t, wet_t, basin_t, dz_wide = state[:7]
    columns, rows = dx_t.shape
    zero = jnp.zeros((SUBLANES, rows), jnp.float32)
    sums = list(sums)
    for start in range(0, per_owner, LEVEL_GROUP):
        group = range(start, min(start + LEVEL_GROUP, per_owner))
        levels = [owner * per_owner + local for local in group]
        velocity_t = [jnp.transpose(velocity_in[level].astype(jnp.float32)) for level in levels]
        theta_t = [jnp.transpose(theta_in[level].astype(jnp.float32)) for level in levels]
        thick_top = [dz_wide[level] for level in levels]
        added = [sums] + [[zero] * (FIELDS * BASINS) for _ in levels[1:]]
        for column in range(0, columns, SUBLANES):
            part = slice(column, column + SUBLANES)
            wet, dx, dxb, basin = wet_t[part, :], dx_t[part, :], dxb_t[part, :], basin_t[part, :]
            flows = []
            for index, level in enumerate(levels):
                width = jnp.where(
                    wet > level + 1, dx, jnp.where(wet == level + 1, dxb, jnp.float32(0.0))
                )
                volume = velocity_t[index][part, :] * (width * thick_top[index])
                flows.append((volume, volume * theta_t[index][part, :]))
            for b in range(BASINS):
                here = basin == b
                for index in range(len(levels)):
                    for field in range(FIELDS):
                        added[index][field * BASINS + b] += jnp.where(
                            here, flows[index][field], jnp.float32(0.0)
                        )
        for index, local in enumerate(group):
            if index:
                sums = [above + own for above, own in zip(sums, added[index])]
            for line in range(FIELDS * BASINS):
                running[pl.ds((line * per_owner + local) * SUBLANES, SUBLANES), :] = sums[line]
    for first in range(0, FIELDS * BASINS * per_owner, SUBLANES):
        total = running[pl.ds(first * SUBLANES, SUBLANES, stride=SUBLANES), :]
        for sublane in range(1, SUBLANES):
            total += running[pl.ds(first * SUBLANES + sublane, SUBLANES, stride=SUBLANES), :]
        piece_ref[pl.ds(first, SUBLANES), :] = total
    return sums


def save_sums(sums_ref, sums):
    for line, value in enumerate(sums):
        sums_ref[line] = value


def first_kernel(
    scale, owners, per_owner, pieces,
    me_ref, dz_hbm, velocity_hbm, theta_hbm, dx_hbm, wet_hbm, bottom_hbm, basin_hbm,
    piece_ref, sums_ref, velocity_in, theta_in, dx_t, dxb_t, wet_t, basin_t, dz_wide, dx_in, dxb_in, wet_in,
    dz_in, bottom_in, basin_in, above, running, sems,
):
    rows, _ = dx_in.shape
    fixed = [
        pltpu.make_async_copy(source, target, sems.at[index])
        for index, (source, target) in enumerate([
            (dz_hbm, dz_in), (dx_hbm, dx_in), (bottom_hbm, bottom_in),
            (wet_hbm, wet_in), (basin_hbm, basin_in),
        ])
    ]

    def level_copies(owner):
        span = pl.ds(owner * per_owner, per_owner)
        return [
            pltpu.make_async_copy(source.at[span], target.at[span], sems.at[len(fixed) + 2 * owner + index])
            for index, (source, target) in enumerate([(velocity_hbm, velocity_in), (theta_hbm, theta_in)])
        ]

    for copy in fixed:
        copy.start()
    for owner in range(owners):
        for copy in level_copies(owner):
            copy.start()
    for copy in fixed:
        copy.wait()
    dx = dx_in[...]
    dxb = dx * (bottom_in[...].astype(jnp.float32) * 0.25)
    dxb_in[...] = dxb
    dx_t[...] = jnp.transpose(dx)
    dxb_t[...] = jnp.transpose(dxb)
    wet_t[...] = jnp.transpose(wet_in[...])
    basin_t[...] = jnp.transpose(basin_in[...])
    for level in range(dz_wide.shape[0]):
        dz_wide[level] = jnp.full(dz_wide.shape[1:], dz_in[level] * scale, jnp.float32)

    state = (velocity_in, theta_in, dx_t, dxb_t, wet_t, basin_t, dz_wide, dx_in, dxb_in, wet_in)
    owner = looked_up(pieces, me_ref[0])

    def wait(owner):
        for copy in level_copies(owner):
            copy.wait()

    zero = jnp.zeros((SUBLANES, rows), jnp.float32)
    save_sums(sums_ref, [zero] * (FIELDS * BASINS))

    @pl.when(owner > 0)
    def _():
        add_above(owner, per_owner, state, above, sums_ref, wait)

    wait(owner)
    sums = [sums_ref[line] for line in range(FIELDS * BASINS)]
    save_sums(sums_ref, one_piece(owner, per_owner, sums, state, running, piece_ref))

    def rest(later, carry):
        wait(later)
        return carry

    lax.fori_loop(owner + 1, owners, rest, 0)


def next_kernel(per_owner, before, pieces, me_ref, sums_in, *refs):
    state, (piece_ref, *sums_ref, running, above, sums_here) = refs[:10], refs[10:]
    owner = looked_up(pieces, me_ref[0])
    follows = owner == looked_up(before, me_ref[0]) + 1
    sums = [jnp.where(follows, sums_in[line], jnp.float32(0.0)) for line in range(FIELDS * BASINS)]
    if any(own not in (0, last + 1) for own, last in zip(pieces, before)):
        save_sums(sums_here, sums)

        @pl.when(jnp.logical_and(owner > 0, jnp.logical_not(follows)))
        def _():
            add_above(owner, per_owner, state, above, sums_here, lambda upper: None)

        sums = [sums_here[line] for line in range(FIELDS * BASINS)]
    sums = one_piece(owner, per_owner, sums, state, running, piece_ref)
    if sums_ref:
        save_sums(sums_ref[0], sums)


def on_device(owners, velocity, theta, dx_cell, wet_levels, bottom_index, basin_id, layer_dz):
    levels, rows, columns = velocity.shape
    scale = 1.0 / (columns * owners) ** 0.5
    per_owner = levels // owners
    lines = FIELDS * BASINS * per_owner
    hbm = pl.BlockSpec(memory_space=pltpu.MemorySpace.HBM)
    vmem = pl.BlockSpec(memory_space=pltpu.VMEM)
    smem = pl.BlockSpec(memory_space=pltpu.SMEM)
    flat = (rows, columns)
    turned = (columns, rows)
    me = lax.axis_index("lon").reshape(1)
    results = [
        pltpu.VMEM((lines, rows), jnp.float32),
        pltpu.VMEM((FIELDS * BASINS, SUBLANES, rows), jnp.float32),
    ]
    running = pltpu.VMEM((lines * SUBLANES, rows), jnp.float32)
    above = pltpu.VMEM((FIELDS,) + flat, jnp.float32)
    sends, pieces = exchange_plan(owners)
    piece, *sums = pl.pallas_call(
        functools.partial(first_kernel, scale, owners, per_owner, tuple(pieces[0])),
        out_shape=results + [
            pltpu.VMEM(velocity.shape, velocity.dtype),
            pltpu.VMEM(theta.shape, theta.dtype),
            pltpu.VMEM(turned, jnp.float32),
            pltpu.VMEM(turned, jnp.float32),
            pltpu.VMEM(turned, jnp.int32),
            pltpu.VMEM(turned, jnp.int32),
            pltpu.VMEM((levels, SUBLANES, rows), jnp.float32),
            pltpu.VMEM(flat, jnp.float32),
            pltpu.VMEM(flat, jnp.float32),
            pltpu.VMEM(flat, jnp.int32),
        ],
        in_specs=[smem] + [hbm] * 7,
        out_specs=[vmem] * 12,
        scratch_shapes=[
            pltpu.SMEM(layer_dz.shape, layer_dz.dtype),
            pltpu.VMEM(flat, jnp.int32),
            pltpu.VMEM(flat, jnp.int32),
            above,
            running,
            pltpu.SemaphoreType.DMA((5 + 2 * owners,)),
        ],
        compiler_params=pltpu.CompilerParams(vmem_limit_bytes=KERNEL_VMEM),
        name="first",
    )(me, *(pltpu.with_memory_space_constraint(x, pltpu.MemorySpace.HBM) for x in (
        layer_dz, velocity, theta, dx_cell, wet_levels, bottom_index, basin_id
    )))
    sums, state = sums[:1], sums[1:]
    arrived = []
    for step in range(1, owners + 1):
        if step > 1:
            kept = 2 if step < owners else 1
            piece, *sums = pl.pallas_call(
                functools.partial(next_kernel, per_owner, tuple(pieces[step - 2]), tuple(pieces[step - 1])),
                out_shape=results[:kept],
                in_specs=[smem] + [vmem] * 11,
                out_specs=[vmem] * kept,
                scratch_shapes=[running, above, results[1]],
                compiler_params=pltpu.CompilerParams(vmem_limit_bytes=KERNEL_VMEM),
                name="following",
            )(me, *(pltpu.with_memory_space_constraint(x, pltpu.VMEM) for x in (*sums, *state)))
        if step < owners:
            arrived.append(lax.ppermute(piece, "lon", sends[step - 1]))
    total = piece
    for other in arrived:
        total = total + other
    return total.reshape(FIELDS, BASINS, per_owner, rows)


def solution(mesh):
    placed = (
        P(None, "lat", "lon"),
        P(None, "lat", "lon"),
        P("lat", "lon"),
        P("lat", "lon"),
        P("lat", "lon"),
        P("lat", "lon"),
        P(),
    )
    owners = mesh.shape["lon"]
    return jax.shard_map(
        functools.partial(on_device, owners),
        mesh=mesh,
        in_specs=placed,
        out_specs=P(None, None, "lon", "lat"),
        check_vma=False,
    )
```

```python
import functools

import jax
import jax.numpy as jnp
from jax import lax
from jax.experimental import pallas as pl
from jax.experimental.pallas import tpu as pltpu
from jax.sharding import PartitionSpec as P


BASINS = 10
FIELDS = 2
SUBLANES = 8
LEVEL_GROUP = 2
KERNEL_VMEM = 16 * 1024 * 1024


def exchange_plan(owners):
    ring = list(range(0, owners, 2)) + list(range(1, owners, 2))
    shifts = []
    for distance in range(1, owners // 2 + 1):
        shifts += sorted({distance, owners - distance})
    sends = [
        [(ring[place], ring[(place + shift) % owners]) for place in range(owners)] for shift in shifts
    ]
    reach, made = [], [0] * owners
    for step in range(owners):
        for device in range(owners):
            needed = sends[step:step + 1] if step else sends[:2]
            wanted = [dict(pairs)[device] + 1 for pairs in needed] if step < owners - 1 else [owners]
            made[device] = max([made[device]] + wanted)
        reach.append(list(made))
    return sends, reach


def slot_of(owner, me, owners):
    low = min if isinstance(owner, int) else jnp.minimum
    half = (owners + 1) // 2
    place = owner // 2 + (owner % 2) * half - me // 2 - (me % 2) * half
    shift = (place + owners) % owners
    near = low(shift, owners - shift)
    slot = 2 * near - 2 + (shift > owners - shift) * 1
    return slot + (shift == 0) * (owners + 1)


def looked_up(table, me):
    found = jnp.int32(table[0])
    for device in range(1, len(table)):
        found = jnp.where(me == device, jnp.int32(table[device]), found)
    return found


def one_piece(owner, per_owner, sums, state, running, slot, piece_refs):
    velocity_in, theta_in, dx_t, dxb_t, wet_t, basin_t, dz_wide = state
    columns, rows = dx_t.shape
    zero = jnp.zeros((SUBLANES, rows), jnp.float32)
    sums = list(sums)
    for start in range(0, per_owner, LEVEL_GROUP):
        group = range(start, min(start + LEVEL_GROUP, per_owner))
        levels = [owner * per_owner + local for local in group]
        velocity_t = [jnp.transpose(velocity_in[level].astype(jnp.float32)) for level in levels]
        theta_t = [jnp.transpose(theta_in[level].astype(jnp.float32)) for level in levels]
        thick_top = [dz_wide[level] for level in levels]
        added = [sums] + [[zero] * (FIELDS * BASINS) for _ in levels[1:]]
        for column in range(0, columns, SUBLANES):
            part = slice(column, column + SUBLANES)
            wet, dx, dxb, basin = wet_t[part, :], dx_t[part, :], dxb_t[part, :], basin_t[part, :]
            flows = []
            for index, level in enumerate(levels):
                width = jnp.where(
                    wet > level + 1, dx, jnp.where(wet == level + 1, dxb, jnp.float32(0.0))
                )
                volume = velocity_t[index][part, :] * (width * thick_top[index])
                flows.append((volume, volume * theta_t[index][part, :]))
            for b in range(BASINS):
                here = basin == b
                for index in range(len(levels)):
                    for field in range(FIELDS):
                        added[index][field * BASINS + b] += jnp.where(
                            here, flows[index][field], jnp.float32(0.0)
                        )
        for index, local in enumerate(group):
            if index:
                sums = [above + own for above, own in zip(sums, added[index])]
            for line in range(FIELDS * BASINS):
                running[pl.ds((line * per_owner + local) * SUBLANES, SUBLANES), :] = sums[line]
    totals = []
    for first in range(0, FIELDS * BASINS * per_owner, SUBLANES):
        total = running[pl.ds(first * SUBLANES, SUBLANES, stride=SUBLANES), :]
        for sublane in range(1, SUBLANES):
            total += running[pl.ds(first * SUBLANES + sublane, SUBLANES, stride=SUBLANES), :]
        totals.append(total)
    for place, piece_ref in piece_refs.items():
        @pl.when(slot == place)
        def _():
            for index, total in enumerate(totals):
                piece_ref[pl.ds(index * SUBLANES, SUBLANES), :] = total
    return sums


def pieces_between(start, stop, me, owners, per_owner, sums, state, running, piece_refs, wait):
    def body(owner, carried):
        wait(owner)
        slot = slot_of(owner, me, owners)
        return tuple(one_piece(owner, per_owner, carried, state, running, slot, piece_refs))

    return lax.fori_loop(start, stop, body, tuple(sums))


def save_sums(sums_ref, sums):
    for line, value in enumerate(sums):
        sums_ref[line] = value


def first_kernel(
    scale, owners, per_owner, reach,
    me_ref, dz_hbm, velocity_hbm, theta_hbm, dx_hbm, wet_hbm, bottom_hbm, basin_hbm,
    *refs,
):
    piece_refs = dict(enumerate(refs[:owners]))
    sums_ref, *state = refs[owners:owners + 8]
    velocity_in, theta_in, dx_t, dxb_t, wet_t, basin_t, dz_wide = state
    dz_in, dx_in, wet_in, bottom_in, basin_in, running, sems = refs[owners + 8:]
    rows, _ = dx_in.shape
    fixed = [
        pltpu.make_async_copy(source, target, sems.at[index])
        for index, (source, target) in enumerate([
            (dz_hbm, dz_in), (dx_hbm, dx_in), (bottom_hbm, bottom_in),
            (wet_hbm, wet_in), (basin_hbm, basin_in),
        ])
    ]

    def level_copies(owner):
        span = pl.ds(owner * per_owner, per_owner)
        return [
            pltpu.make_async_copy(source.at[span], target.at[span], sems.at[len(fixed) + 2 * owner + index])
            for index, (source, target) in enumerate([(velocity_hbm, velocity_in), (theta_hbm, theta_in)])
        ]

    for copy in fixed:
        copy.start()
    for owner in range(owners):
        for copy in level_copies(owner):
            copy.start()
    for copy in fixed:
        copy.wait()
    dx = dx_in[...]
    dxb = dx * (bottom_in[...].astype(jnp.float32) * 0.25)
    dx_t[...] = jnp.transpose(dx)
    dxb_t[...] = jnp.transpose(dxb)
    wet_t[...] = jnp.transpose(wet_in[...])
    basin_t[...] = jnp.transpose(basin_in[...])
    for level in range(dz_wide.shape[0]):
        dz_wide[level] = jnp.full(dz_wide.shape[1:], dz_in[level] * scale, jnp.float32)

    def wait(owner):
        for copy in level_copies(owner):
            copy.wait()

    me = me_ref[0]
    stop = looked_up(reach, me)
    zero = jnp.zeros((SUBLANES, rows), jnp.float32)
    save_sums(sums_ref, pieces_between(
        0, stop, me, owners, per_owner, (zero,) * (FIELDS * BASINS), state, running, piece_refs, wait
    ))

    def rest(later, carry):
        wait(later)
        return carry

    lax.fori_loop(stop, owners, rest, 0)


def next_kernel(owners, per_owner, before, reach, slots, me_ref, sums_in, *refs):
    count = len(slots)
    state = refs[count:count + 7]
    piece_refs = dict(zip(slots, refs[count + 7:]))
    *sums_ref, running = refs[2 * count + 7:]
    me = me_ref[0]
    sums = pieces_between(
        looked_up(before, me), looked_up(reach, me), me, owners, per_owner,
        [sums_in[line] for line in range(FIELDS * BASINS)], state, running, piece_refs, lambda owner: None,
    )
    if sums_ref:
        save_sums(sums_ref[0], sums)


def on_device(owners, velocity, theta, dx_cell, wet_levels, bottom_index, basin_id, layer_dz):
    levels, rows, columns = velocity.shape
    scale = 1.0 / (columns * owners) ** 0.5
    per_owner = levels // owners
    lines = FIELDS * BASINS * per_owner
    hbm = pl.BlockSpec(memory_space=pltpu.MemorySpace.HBM)
    vmem = pl.BlockSpec(memory_space=pltpu.VMEM)
    smem = pl.BlockSpec(memory_space=pltpu.SMEM)
    flat = (rows, columns)
    turned = (columns, rows)
    me = lax.axis_index("lon").reshape(1)
    whole_piece = pltpu.VMEM((lines, rows), jnp.float32)
    all_sums = pltpu.VMEM((FIELDS * BASINS, SUBLANES, rows), jnp.float32)
    running = pltpu.VMEM((lines * SUBLANES, rows), jnp.float32)
    limit = pltpu.CompilerParams(vmem_limit_bytes=KERNEL_VMEM)

    def placed_in(space, arrays):
        return [pltpu.with_memory_space_constraint(array, space) for array in arrays]

    sends, reach = exchange_plan(owners)
    *pieces, sums, velocity_in, theta_in, dx_t, dxb_t, wet_t, basin_t, dz_wide = pl.pallas_call(
        functools.partial(first_kernel, scale, owners, per_owner, tuple(reach[0])),
        out_shape=[whole_piece] * owners + [
            all_sums,
            pltpu.VMEM(velocity.shape, velocity.dtype),
            pltpu.VMEM(theta.shape, theta.dtype),
            pltpu.VMEM(turned, jnp.float32),
            pltpu.VMEM(turned, jnp.float32),
            pltpu.VMEM(turned, jnp.int32),
            pltpu.VMEM(turned, jnp.int32),
            pltpu.VMEM((levels, SUBLANES, rows), jnp.float32),
        ],
        in_specs=[smem] + [hbm] * 7,
        out_specs=[vmem] * (owners + 8),
        scratch_shapes=[
            pltpu.SMEM(layer_dz.shape, layer_dz.dtype),
            pltpu.VMEM(flat, jnp.float32),
            pltpu.VMEM(flat, jnp.int32),
            pltpu.VMEM(flat, jnp.int32),
            pltpu.VMEM(flat, jnp.int32),
            running,
            pltpu.SemaphoreType.DMA((5 + 2 * owners,)),
        ],
        compiler_params=limit,
        name="first",
    )(me, *placed_in(pltpu.MemorySpace.HBM, (layer_dz, velocity, theta, dx_cell, wet_levels, bottom_index, basin_id)))
    state = (velocity_in, theta_in, dx_t, dxb_t, wet_t, basin_t, dz_wide)
    arrived = []
    for step in range(1, owners + 1):
        before, now = reach[max(step - 2, 0)], reach[step - 1]
        slots = sorted({
            slot_of(owner, device, owners)
            for device in range(owners) for owner in range(before[device], now[device])
        })
        if slots:
            last = 1 if step < owners else 0
            made = list(pl.pallas_call(
                functools.partial(
                    next_kernel, owners, per_owner, tuple(before), tuple(now), tuple(slots)
                ),
                out_shape=[whole_piece] * len(slots) + [all_sums] * last,
                in_specs=[smem] + [vmem] * (len(slots) + 8),
                out_specs=[vmem] * (len(slots) + last),
                scratch_shapes=[running],
                input_output_aliases={2 + index: index for index in range(len(slots))},
                compiler_params=limit,
                name="following",
            )(me, *placed_in(pltpu.VMEM, [sums] + [pieces[slot] for slot in slots] + list(state))))
            if last:
                sums = made.pop()
            for slot, piece in zip(slots, made):
                pieces[slot] = piece
        if step < owners:
            arrived.append(lax.ppermute(pieces[step - 1], "lon", sends[step - 1]))
    total = pieces[owners - 1]
    for other in arrived:
        total = total + other
    return total.reshape(FIELDS, BASINS, per_owner, rows)


def solution(mesh):
    placed = (
        P(None, "lat", "lon"),
        P(None, "lat", "lon"),
        P("lat", "lon"),
        P("lat", "lon"),
        P("lat", "lon"),
        P("lat", "lon"),
        P(),
    )
    owners = mesh.shape["lon"]
    _, _ = exchange_plan(owners)
    return jax.shard_map(
        functools.partial(on_device, owners),
        mesh=mesh,
        in_specs=placed,
        out_specs=P(None, None, "lon", "lat"),
        check_vma=False,
    )
```

```python
import functools

import jax
import jax.numpy as jnp
from jax import lax
from jax.experimental import pallas as pl
from jax.experimental.pallas import tpu as pltpu
from jax.sharding import PartitionSpec as P


BASINS = 10
FIELDS = 2
SUBLANES = 8
LEVEL_GROUP = 2
KERNEL_VMEM = 16 * 1024 * 1024


def exchange_plan(owners):
    ring = list(range(0, owners, 2)) + list(range(1, owners, 2))
    shifts = []
    for distance in range(1, owners // 2 + 1):
        shifts += sorted({distance, owners - distance})
    sends = [
        [(ring[place], ring[(place + shift) % owners]) for place in range(owners)] for shift in shifts
    ]
    starts, stops = [[0] * owners for _ in range(owners)], [[0] * owners for _ in range(owners)]
    for device in range(owners):
        wanted = [dict(pairs)[device] for pairs in sends] + [device]
        made, place = set(), 0
        for step, owner in enumerate(wanted):
            start = stop = place
            if step == 0:
                start, stop = min(wanted[:2]), max(wanted[:2]) + 1
                if device == 0:
                    start, stop = 0, owners
            elif owner not in made:
                start, stop = owner, owner + 1
            made.update(range(start, stop))
            place = stop
            starts[step][device], stops[step][device] = start, stop
    return sends, starts, stops


def slot_of(owner, me, owners):
    low = min if isinstance(owner, int) else jnp.minimum
    half = (owners + 1) // 2
    place = owner // 2 + (owner % 2) * half - me // 2 - (me % 2) * half
    shift = (place + owners) % owners
    near = low(shift, owners - shift)
    slot = 2 * near - 2 + (shift > owners - shift) * 1
    return slot + (shift == 0) * (owners + 1)


def looked_up(table, me):
    found = jnp.int32(table[0])
    for device in range(1, len(table)):
        found = jnp.where(me == device, jnp.int32(table[device]), found)
    return found


def add_above(owner, per_owner, state, above, sums_ref, wait):
    velocity_in, theta_in, _, _, _, basin_t, dz_wide, dx_in, dxb_in, wet_in = state
    rows, columns = dx_in.shape
    block = 2 * SUBLANES
    for field in range(FIELDS):
        above[field] = jnp.zeros((rows, columns), jnp.float32)

    def add_owner(upper, carry):
        wait(upper)
        for row in range(0, rows, block):
            part = slice(row, row + block)
            wet, dx, dxb = wet_in[part, :], dx_in[part, :], dxb_in[part, :]
            volumes, heats = above[0, part, :], above[1, part, :]
            for local in range(per_owner):
                level = upper * per_owner + local
                width = jnp.where(
                    wet > level + 1, dx, jnp.where(wet == level + 1, dxb, jnp.float32(0.0))
                )
                volume = velocity_in[level, part, :].astype(jnp.float32) * (width * dz_wide[level, 0:1, 0:1])
                volumes += volume
                heats += volume * theta_in[level, part, :].astype(jnp.float32)
            above[0, part, :] = volumes
            above[1, part, :] = heats
        return carry

    lax.fori_loop(0, owner, add_owner, 0)
    sums = [jnp.zeros((SUBLANES, rows), jnp.float32)] * (FIELDS * BASINS)
    flows = [jnp.transpose(above[field]) for field in range(FIELDS)]
    for column in range(0, columns, SUBLANES):
        part = slice(column, column + SUBLANES)
        for b in range(BASINS):
            here = basin_t[part, :] == b
            for field in range(FIELDS):
                sums[field * BASINS + b] += jnp.where(here, flows[field][part, :], jnp.float32(0.0))
    save_sums(sums_ref, sums)


def one_piece(owner, per_owner, sums, state, running, slot, piece_refs):
    velocity_in, theta_in, dx_t, dxb_t, wet_t, basin_t, dz_wide = state[:7]
    columns, rows = dx_t.shape
    zero = jnp.zeros((SUBLANES, rows), jnp.float32)
    sums = list(sums)
    for start in range(0, per_owner, LEVEL_GROUP):
        group = range(start, min(start + LEVEL_GROUP, per_owner))
        levels = [owner * per_owner + local for local in group]
        velocity_t = [jnp.transpose(velocity_in[level].astype(jnp.float32)) for level in levels]
        theta_t = [jnp.transpose(theta_in[level].astype(jnp.float32)) for level in levels]
        thick_top = [dz_wide[level] for level in levels]
        added = [sums] + [[zero] * (FIELDS * BASINS) for _ in levels[1:]]
        for column in range(0, columns, SUBLANES):
            part = slice(column, column + SUBLANES)
            wet, dx, dxb, basin = wet_t[part, :], dx_t[part, :], dxb_t[part, :], basin_t[part, :]
            flows = []
            for index, level in enumerate(levels):
                width = jnp.where(
                    wet > level + 1, dx, jnp.where(wet == level + 1, dxb, jnp.float32(0.0))
                )
                volume = velocity_t[index][part, :] * (width * thick_top[index])
                flows.append((volume, volume * theta_t[index][part, :]))
            for b in range(BASINS):
                here = basin == b
                for index in range(len(levels)):
                    for field in range(FIELDS):
                        added[index][field * BASINS + b] += jnp.where(
                            here, flows[index][field], jnp.float32(0.0)
                        )
        for index, local in enumerate(group):
            if index:
                sums = [above + own for above, own in zip(sums, added[index])]
            for line in range(FIELDS * BASINS):
                running[pl.ds((line * per_owner + local) * SUBLANES, SUBLANES), :] = sums[line]
    totals = []
    for first in range(0, FIELDS * BASINS * per_owner, SUBLANES):
        total = running[pl.ds(first * SUBLANES, SUBLANES, stride=SUBLANES), :]
        for sublane in range(1, SUBLANES):
            total += running[pl.ds(first * SUBLANES + sublane, SUBLANES, stride=SUBLANES), :]
        totals.append(total)
    for place, piece_ref in piece_refs.items():
        @pl.when(slot == place)
        def _():
            for index, total in enumerate(totals):
                piece_ref[pl.ds(index * SUBLANES, SUBLANES), :] = total
    return sums


def pieces_between(start, stop, me, owners, per_owner, sums, state, running, piece_refs, wait):
    def body(owner, carried):
        wait(owner)
        slot = slot_of(owner, me, owners)
        return tuple(one_piece(owner, per_owner, carried, state, running, slot, piece_refs))

    return lax.fori_loop(start, stop, body, tuple(sums))


def save_sums(sums_ref, sums):
    for line, value in enumerate(sums):
        sums_ref[line] = value


def first_kernel(
    scale, owners, per_owner, starts, stops,
    me_ref, dz_hbm, velocity_hbm, theta_hbm, dx_hbm, wet_hbm, bottom_hbm, basin_hbm,
    *refs,
):
    piece_refs = dict(enumerate(refs[:owners]))
    sums_ref, *state = refs[owners:owners + 11]
    velocity_in, theta_in, dx_t, dxb_t, wet_t, basin_t, dz_wide, dx_in, dxb_in, wet_in = state
    dz_in, bottom_in, basin_in, above, running, sems = refs[owners + 11:]
    rows, _ = dx_in.shape
    fixed = [
        pltpu.make_async_copy(source, target, sems.at[index])
        for index, (source, target) in enumerate([
            (dz_hbm, dz_in), (dx_hbm, dx_in), (bottom_hbm, bottom_in),
            (wet_hbm, wet_in), (basin_hbm, basin_in),
        ])
    ]

    def level_copies(owner):
        span = pl.ds(owner * per_owner, per_owner)
        return [
            pltpu.make_async_copy(source.at[span], target.at[span], sems.at[len(fixed) + 2 * owner + index])
            for index, (source, target) in enumerate([(velocity_hbm, velocity_in), (theta_hbm, theta_in)])
        ]

    for copy in fixed:
        copy.start()
    for owner in range(owners):
        for copy in level_copies(owner):
            copy.start()
    for copy in fixed:
        copy.wait()
    dx = dx_in[...]
    dxb = dx * (bottom_in[...].astype(jnp.float32) * 0.25)
    dxb_in[...] = dxb
    dx_t[...] = jnp.transpose(dx)
    dxb_t[...] = jnp.transpose(dxb)
    wet_t[...] = jnp.transpose(wet_in[...])
    basin_t[...] = jnp.transpose(basin_in[...])
    for level in range(dz_wide.shape[0]):
        dz_wide[level] = jnp.full(dz_wide.shape[1:], dz_in[level] * scale, jnp.float32)

    def wait(owner):
        for copy in level_copies(owner):
            copy.wait()

    me = me_ref[0]
    start, stop = looked_up(starts, me), looked_up(stops, me)
    zero = jnp.zeros((SUBLANES, rows), jnp.float32)
    save_sums(sums_ref, [zero] * (FIELDS * BASINS))

    @pl.when(start > 0)
    def _():
        add_above(start, per_owner, state, above, sums_ref, wait)

    save_sums(sums_ref, pieces_between(
        start, stop, me, owners, per_owner, [sums_ref[line] for line in range(FIELDS * BASINS)],
        state, running, piece_refs, wait,
    ))

    def rest(later, carry):
        wait(later)
        return carry

    lax.fori_loop(stop, owners, rest, 0)


def next_kernel(owners, per_owner, before, starts, stops, slots, me_ref, sums_in, *refs):
    count = len(slots)
    state = refs[count:count + 10]
    piece_refs = dict(zip(slots, refs[count + 10:]))
    *sums_ref, running, above, sums_here = refs[2 * count + 10:]
    me = me_ref[0]
    start, stop = looked_up(starts, me), looked_up(stops, me)
    follows = start == looked_up(before, me)
    sums = [jnp.where(follows, sums_in[line], jnp.float32(0.0)) for line in range(FIELDS * BASINS)]
    if any(own not in (0, last) for own, last in zip(starts, before)):
        save_sums(sums_here, sums)

        @pl.when(jnp.logical_and(start > 0, jnp.logical_not(follows)))
        def _():
            add_above(start, per_owner, state, above, sums_here, lambda owner: None)

        sums = [sums_here[line] for line in range(FIELDS * BASINS)]
    sums = pieces_between(
        start, stop, me, owners, per_owner, sums, state, running, piece_refs, lambda owner: None
    )
    if sums_ref:
        save_sums(sums_ref[0], sums)


def on_device(owners, velocity, theta, dx_cell, wet_levels, bottom_index, basin_id, layer_dz):
    levels, rows, columns = velocity.shape
    scale = 1.0 / (columns * owners) ** 0.5
    per_owner = levels // owners
    lines = FIELDS * BASINS * per_owner
    hbm = pl.BlockSpec(memory_space=pltpu.MemorySpace.HBM)
    vmem = pl.BlockSpec(memory_space=pltpu.VMEM)
    smem = pl.BlockSpec(memory_space=pltpu.SMEM)
    flat = (rows, columns)
    turned = (columns, rows)
    me = lax.axis_index("lon").reshape(1)
    whole_piece = pltpu.VMEM((lines, rows), jnp.float32)
    all_sums = pltpu.VMEM((FIELDS * BASINS, SUBLANES, rows), jnp.float32)
    running = pltpu.VMEM((lines * SUBLANES, rows), jnp.float32)
    limit = pltpu.CompilerParams(vmem_limit_bytes=KERNEL_VMEM)

    def placed_in(space, arrays):
        return [pltpu.with_memory_space_constraint(array, space) for array in arrays]

    above = pltpu.VMEM((FIELDS,) + flat, jnp.float32)
    sends, starts, stops = exchange_plan(owners)
    *pieces, sums, velocity_in, theta_in, dx_t, dxb_t, wet_t, basin_t, dz_wide, dx_in, dxb_in, wet_in = pl.pallas_call(
        functools.partial(first_kernel, scale, owners, per_owner, tuple(starts[0]), tuple(stops[0])),
        out_shape=[whole_piece] * owners + [
            all_sums,
            pltpu.VMEM(velocity.shape, velocity.dtype),
            pltpu.VMEM(theta.shape, theta.dtype),
            pltpu.VMEM(turned, jnp.float32),
            pltpu.VMEM(turned, jnp.float32),
            pltpu.VMEM(turned, jnp.int32),
            pltpu.VMEM(turned, jnp.int32),
            pltpu.VMEM((levels, SUBLANES, rows), jnp.float32),
            pltpu.VMEM(flat, jnp.float32),
            pltpu.VMEM(flat, jnp.float32),
            pltpu.VMEM(flat, jnp.int32),
        ],
        in_specs=[smem] + [hbm] * 7,
        out_specs=[vmem] * (owners + 11),
        scratch_shapes=[
            pltpu.SMEM(layer_dz.shape, layer_dz.dtype),
            pltpu.VMEM(flat, jnp.int32),
            pltpu.VMEM(flat, jnp.int32),
            above,
            running,
            pltpu.SemaphoreType.DMA((5 + 2 * owners,)),
        ],
        compiler_params=limit,
        name="first",
    )(me, *placed_in(pltpu.MemorySpace.HBM, (layer_dz, velocity, theta, dx_cell, wet_levels, bottom_index, basin_id)))
    state = (velocity_in, theta_in, dx_t, dxb_t, wet_t, basin_t, dz_wide, dx_in, dxb_in, wet_in)
    arrived = []
    for step in range(1, owners + 1):
        start, stop = starts[step - 1], stops[step - 1]
        slots = sorted({
            slot_of(owner, device, owners)
            for device in range(owners) for owner in range(start[device], stop[device])
        })
        if step > 1 and slots:
            last = 1 if step < owners else 0
            made = list(pl.pallas_call(
                functools.partial(
                    next_kernel, owners, per_owner, tuple(stops[step - 2]), tuple(start), tuple(stop), tuple(slots)
                ),
                out_shape=[whole_piece] * len(slots) + [all_sums] * last,
                in_specs=[smem] + [vmem] * (len(slots) + 11),
                out_specs=[vmem] * (len(slots) + last),
                scratch_shapes=[running, above, all_sums],
                input_output_aliases={2 + index: index for index in range(len(slots))},
                compiler_params=limit,
                name="following",
            )(me, *placed_in(pltpu.VMEM, [sums] + [pieces[slot] for slot in slots] + list(state))))
            if last:
                sums = made.pop()
            for slot, piece in zip(slots, made):
                pieces[slot] = piece
        if step < owners:
            arrived.append(lax.ppermute(pieces[step - 1], "lon", sends[step - 1]))
    total = pieces[owners - 1]
    for other in arrived:
        total = total + other
    return total.reshape(FIELDS, BASINS, per_owner, rows)


def solution(mesh):
    placed = (
        P(None, "lat", "lon"),
        P(None, "lat", "lon"),
        P("lat", "lon"),
        P("lat", "lon"),
        P("lat", "lon"),
        P("lat", "lon"),
        P(),
    )
    owners = mesh.shape["lon"]
    _, _, _ = exchange_plan(owners)
    return jax.shard_map(
        functools.partial(on_device, owners),
        mesh=mesh,
        in_specs=placed,
        out_specs=P(None, None, "lon", "lat"),
        check_vma=False,
    )
```
